32 devices in a mesh: gx: 8 (over z, x), gy: 4 (over y, core).
Axes of the slice: x: 2, y: 2, z: 4, core: 2. Of those that a mesh axis runs over, the one named last changes fastest.
Arguments:
- parcel_props: float32 [16, 131072], P(None, ('gx', 'gy')), may hold values from -6 to 6
- size_class: int32 [131072], P(('gx', 'gy')), may hold values from 0 to 7
- dest_owner: int32 [131072, 1], P(('gx', 'gy')), may hold values from 0 to 31; in each aligned block of 4096 rows (0 to 4095, 4096 to 8191, ...) at most 512 rows name the same one
- dest_local: int32 [131072], P(('gx', 'gy')), may hold values from 0 to 4095
- class_table: float32 [8, 16], replicated, may hold values from 0.5 to 2
- gas_density: float32 [256, 512], P('gx', 'gy'), may hold values from 0.5 to 2
- gas_rest: float32 [4, 256, 512], P(None, 'gx', 'gy'), may hold values from -6 to 6
Outputs:
- new_density: float32 [256, 512], P('gx', 'gy')
- new_rest: float32 [4, 256, 512], P(None, 'gx', 'gy')
The draws below stay inside these ranges and needn't reach their ends.
Inputs may be any that keep to these rules, and one draw needn't show every extreme that they name: `dest_owner`: among the parcels of one device, no owner device is named by more than 512 of them, a bound that some block reaches.
All inputs are finite; a program needn't handle non-finite values.
Results may differ from the reference program's by a relative error of at most 0.00015.
Values sent between devices are 32-bit elements; how exact they have to be, the bound alone decides.
A program may use at most 64 MiB of HBM per device.

```python
import math
import jax
import jax.numpy as jnp
import numpy as np
from jax import lax

PROPS = 16
CLASSES = 8
PARC_DEV = 4096
LX = 32
LY = 128
CAP = 512
PARCELS = 131072
NX = 256
NY = 512
N_GY = 4
DEVICES = 32


def place_ends(drawn, rng, least, high):
    longest = drawn.shape.index(max(drawn.shape))
    spots = []
    for shift in (0, 1):
        where = [jax.random.randint(jax.random.fold_in(rng, axis), (), 0, length) for axis, length in enumerate(drawn.shape)]
        where[longest] = (where[longest] + shift) % drawn.shape[longest]
        spots.append(tuple(where))
    return drawn.at[spots[0]].set(least).at[spots[1]].set(high)


def steps_of(own_key, shape, shards, least, largest):
    def one(axis_at, shards_of):
        heights = jax.random.uniform(jax.random.fold_in(jax.random.fold_in(own_key, 6), axis_at), (shards_of,), jnp.float32, least / len(shards), largest / len(shards))
        return jnp.repeat(jnp.exp(heights), shape[axis_at] // shards_of).reshape((-1,) + (1,) * (len(shape) - axis_at - 1))

    level = one(*shards[0])
    for cut in shards[1:]:
        level = level * one(*cut)
    return level


def routed_block(key, own, number, rows, count, top, limit, lean):
    sequence = jax.random.permutation(key, count)
    packed, common = load_shares(count, rows * top, limit, lean, True), load_shares(count, rows * top, limit, lean, False)
    places = jnp.arange(count)

    def named(tallies, rotation):
        used = int((tallies > 0).sum())
        fixed = max(1, used // 4)
        shifted = fixed + (places - fixed + rotation * (used - fixed)) % max(1, count - fixed)
        return jnp.zeros((count,), jnp.int32).at[sequence[jnp.where(places < fixed, places, shifted)]].set(jnp.asarray(tallies, jnp.int32))

    tallies = jnp.where(number % 4 == 0, named(packed, number // 4), named(common, number - number // 4 - 1))
    mixed = jax.random.permutation(jax.random.fold_in(own, 3), count)
    source_of, sink = mixed[0:count // 2 * 2:2], mixed[1:count // 2 * 2:2]
    margin = jnp.minimum(tallies[source_of] - 1, limit - tallies[sink]) // 2
    margin = jnp.where((source_of == sequence[0]) | (sink == sequence[0]) | (tallies[sink] == 0), 0, jnp.maximum(margin, 0))
    shifted = jax.random.randint(jax.random.fold_in(own, 4), (count // 2,), 0, 1 << 20) % (margin + 1)
    tallies = tallies.at[source_of].add(-shifted).at[sink].add(shifted)
    members = jnp.searchsorted(jnp.cumsum(tallies), jnp.arange(rows * top), side="right").astype(jnp.int32)
    table = members.reshape(top, rows).T
    table = table[jax.random.permutation(jax.random.fold_in(own, 1), rows)]
    rotation = jax.random.randint(jax.random.fold_in(own, 2), (rows, 1), 0, top)
    return jnp.take_along_axis(table, (jnp.arange(top)[None, :] + rotation) % top, axis=1)


def load_shares(count, total, most, lean, full):
    weights = [(1 << 20) // math.isqrt(standing ** lean) + 1 for standing in range(1, count + 1)]
    largest = most if full else min(most, max(-(-total // count), total * weights[0] // sum(weights)))
    least = 1 if total - largest >= count - 1 else 0
    holding, surplus = [largest] + [least] * (count - 1), total - largest - least * (count - 1)
    while surplus > 0:
        free = [i for i in range(1, count) if holding[i] < largest] or [i for i in range(1, count) if holding[i] < most]
        whole, left = sum([weights[i] for i in free]), surplus
        for i in free:
            more = min(most - holding[i], max(1, left * weights[i] // whole), surplus)
            holding[i] = holding[i] + more
            surplus = surplus - more
    return np.array(holding)


def bell_draw(key, extent, width, most, cuts=(), kind=jnp.bfloat16):
    array = width * jax.random.normal(key, extent, jnp.float32)
    if cuts:
        array = array * steps_of(key, extent, cuts, -0.22, 0.18)
    return jnp.clip(array, -most, most).astype(kind)


def setup_inputs(seed: int = 0) -> dict:
    seeds = jax.random.split(jax.random.key(seed), 8)
    parcel_props = bell_draw(seeds[0], (PROPS, PARCELS), 1.0, 6.0, ((1, 32),), jnp.float32)
    size_class = place_ends(jax.random.randint(seeds[1], (PARCELS,), 0, CLASSES), jax.random.fold_in(seeds[1], 1), 0, CLASSES - 1).astype(jnp.int32)
    dest_owner_keys = jax.random.split(jax.random.fold_in(seeds[2], 1), PARCELS // PARC_DEV)
    dest_owner_turns = jax.random.permutation(jax.random.fold_in(seeds[2], 3), PARCELS // PARC_DEV)
    dest_owner = jax.vmap(lambda own, number: routed_block(jax.random.fold_in(seeds[2], 2), own, number, PARC_DEV, DEVICES, 1, CAP, 2))(dest_owner_keys, dest_owner_turns).reshape((PARCELS, 1))
    dest_local = place_ends(jax.random.randint(seeds[3], (PARCELS,), 0, LX * LY), jax.random.fold_in(seeds[3], 1), 0, (LX * LY) - 1).astype(jnp.int32)
    class_table = jnp.clip(jnp.exp(jax.random.uniform(seeds[4], (CLASSES, PROPS), jnp.float32, math.log(0.5), math.log(2.0))), 0.5, 2.0)
    gas_density = jnp.clip(jnp.exp(math.log(2.0) - 1.3862944 * jax.random.uniform(seeds[5], (NX, NY), jnp.float32) ** steps_of(seeds[5], (NX, NY), ((0, 8), (1, 4)), -0.2, 0.2)), 0.5, 2.0)
    gas_rest = bell_draw(seeds[6], (4, NX, NY), 1.0, 6.0, ((1, 8), (2, 4)), jnp.float32)
    return dict(parcel_props=parcel_props, size_class=size_class, dest_owner=dest_owner, dest_local=dest_local, class_table=class_table, gas_density=gas_density, gas_rest=gas_rest)


def sources_of(props, classes, gas, table):
    picks = (classes[None, :] == jnp.arange(CLASSES, dtype=jnp.int32)[:, None]).astype(jnp.float32)
    coef = jnp.dot(table.T, picks, precision=lax.Precision.HIGHEST, preferred_element_type=jnp.float32)
    mass = jnp.exp(0.5 * props[0])
    density = gas[0]
    velocity = gas[1:4] / density
    theta = gas[4] / density
    slip = props[1:4] - velocity
    rate = coef[0] * jax.nn.softplus(props[4] - theta)
    evapor = mass * (1.0 - jnp.exp(-rate))
    dragged = 1.0 - jnp.exp(-coef[1] * jnp.sqrt(1.0 + lax.optimization_barrier(jnp.sum(slip * slip, axis=0))))
    moment = evapor * coef[2:5] * props[1:4] + mass * dragged * slip
    energy = evapor * (props[4] + lax.optimization_barrier(jnp.sum(coef[5:] * props[5:], axis=0)))
    return jnp.concatenate([evapor[None], moment, energy[None]], axis=0)

def smooth_field(deposit):
    padded = jnp.pad(deposit, ((0, 0), (1, 1), (1, 1)))
    beside = padded[:, 2:, 1:-1] + padded[:, :-2, 1:-1] + padded[:, 1:-1, 2:] + padded[:, 1:-1, :-2]
    return 0.4 * deposit + 0.15 * beside

def reference(parcel_props, size_class, dest_owner, dest_local, class_table, gas_density, gas_rest):
    owner = dest_owner[:, 0]
    cell_x = owner // N_GY * LX + dest_local // LY
    cell_y = owner % N_GY * LY + dest_local % LY
    flat = (cell_x * NY + cell_y).astype(jnp.int32)
    gas = jnp.concatenate([gas_density[None], gas_rest], axis=0).reshape(5, NX * NY)
    local_gas = gas[:, flat]
    source = sources_of(parcel_props, size_class, local_gas, class_table)
    deposit = jnp.zeros((5, NX * NY), jnp.float32).at[:, flat].add(source).reshape(5, NX, NY)
    smooth = smooth_field(deposit)
    return (gas_density + smooth[0], gas_rest + smooth[1:])
```

```python
import functools

import jax
import jax.numpy as jnp
from jax import lax
from jax.experimental import pallas as pl
from jax.experimental.pallas import tpu as pltpu
from jax.sharding import PartitionSpec as P

F32 = jnp.float32
BF16 = jnp.bfloat16
LANES = 128
ROWS = 8
NT = (((1,), (1,)), ((), ()))


def split(x):
    high = x.astype(BF16).astype(F32)
    return high, x - high


def iota(shape, dim):
    return lax.broadcasted_iota(jnp.int32, shape, dim)


def bucket_kernel(
    devices, capacity, props_ref, class_ref, owner_ref, cell_ref, table_ref, out_ref, hot, vals
):
    props_count, parcels = props_ref.shape
    classes = table_ref.shape[0]
    chunks = parcels // LANES

    row, col = (iota((LANES, 2 * LANES), 0), iota((LANES, 2 * LANES), 1))
    upper = jnp.where((col >= LANES) | (row < col), 1.0, 0.0).astype(BF16)
    ids = iota((devices, LANES), 0)
    ranks = iota((capacity, LANES), 0)

    def member(c):
        return owner_ref[:, c * LANES : (c + 1) * LANES] == ids

    carry = jnp.zeros((devices, LANES), F32)
    for c in range(chunks):
        mine = member(c)
        counted = jnp.dot(
            jnp.where(mine, 1.0, 0.0).astype(BF16), upper, preferred_element_type=F32
        )
        rank = jnp.sum(
            jnp.where(mine, counted[:, :LANES] + carry, 0.0), axis=0, keepdims=True
        ).astype(jnp.int32)
        carry = carry + counted[:, LANES:]
        hot[:, c * LANES : (c + 1) * LANES] = jnp.where(ranks == rank, 1.0, 0.0).astype(BF16)

    eye = jnp.where(
        iota((props_count, props_count), 0) == iota((props_count, props_count), 1), 1.0, 0.0
    ).astype(BF16)
    table = jnp.concatenate(split(table_ref[...]), axis=0).astype(BF16)
    turned = lax.dot_general(eye, table, NT, preferred_element_type=F32).astype(BF16)
    picks = jnp.where(class_ref[...] == iota((classes, parcels), 0), 1.0, 0.0)
    picks = jnp.concatenate([picks, picks], axis=0).astype(BF16)
    coef = jnp.dot(turned, picks, preferred_element_type=F32)
    props = props_ref[...]
    which = iota((props_count, parcels), 0)
    weights = jnp.where(which >= 5, coef, jnp.where(which == 4, 1.0, 0.0))
    heat = jnp.sum(weights * props, axis=0, keepdims=True)
    which = iota((ROWS, parcels), 0)
    mixed = jnp.where(which == 0, jnp.exp(0.5 * props[0:1]), props[0:ROWS])
    mixed = jnp.where(which == 5, heat, mixed)
    mixed = jnp.where(which == 6, class_ref[...].astype(F32), mixed)
    mixed = jnp.where(which == 7, cell_ref[...].astype(F32), mixed)
    vals[...] = jnp.concatenate(split(mixed), axis=0)

    def group(g, unused):
        sends = [
            jnp.where(owner_ref[...] == g * ROWS + i, vals[...], 0.0).astype(BF16)
            for i in range(ROWS)
        ]
        packed = lax.dot_general(
            jnp.concatenate(sends, axis=0), hot[...], NT, preferred_element_type=F32
        )
        for i in range(ROWS):
            first = 2 * ROWS * i
            out_ref[g * ROWS + i] = (
                packed[first : first + ROWS] + packed[first + ROWS : first + 2 * ROWS]
            )
        return unused

    lax.fori_loop(0, devices // ROWS, group, 0)


def deposit_kernel(devices, capacity, got_ref, table_ref, dens_ref, rest_ref, out_ref, spot, gas, src, total):
    slab_x, slab_y = dens_ref.shape
    classes = table_ref.shape[0]
    fields = jnp.concatenate([dens_ref[...], rest_ref[...].reshape(4 * slab_x, slab_y)], axis=0)
    tab = jnp.concatenate(split(fields), axis=1).astype(BF16)
    total[...] = jnp.zeros_like(total)
    ys = iota((slab_y, capacity), 0)
    xs = iota((slab_x, capacity), 0)

    def group(g, unused):
        def cell_of(i):
            return got_ref[(g * ROWS + i)][7:8].astype(jnp.int32)

        def part(c):
            return jnp.concatenate([got_ref[g * ROWS + i][c : c + 1] for i in range(ROWS)], axis=0)

        for i in range(ROWS):
            cell = cell_of(i)
            hot = jnp.where(ys == cell % slab_y, 1.0, 0.0).astype(BF16)
            spot[:, i * capacity : (i + 1) * capacity] = hot
            found = jnp.dot(tab, jnp.concatenate([hot, hot], axis=0), preferred_element_type=F32)
            in_row = xs == cell // slab_y
            for c in range(5):
                gas[c, i : i + 1] = jnp.sum(
                    jnp.where(in_row, found[c * slab_x : (c + 1) * slab_x], 0.0),
                    axis=0,
                    keepdims=True,
                )

        kind = part(6).astype(jnp.int32)
        coef = [jnp.full(kind.shape, table_ref[0, j], F32) for j in range(5)]
        for k in range(1, classes):
            same = kind == k
            coef = [jnp.where(same, table_ref[k, j], coef[j]) for j in range(5)]
        mass = part(0)
        speed = [part(j) for j in (1, 2, 3)]
        heat, energy = part(4), part(5)
        inverse = 1.0 / gas[0]
        slip = [speed[j] - gas[j + 1] * inverse for j in range(3)]
        excess = heat - gas[4] * inverse
        soft = jnp.maximum(excess, 0.0) + jnp.log1p(jnp.exp(-jnp.abs(excess)))
        evapor = mass * (1.0 - jnp.exp(-(coef[0] * soft)))
        square = slip[0] * slip[0] + slip[1] * slip[1] + slip[2] * slip[2]
        drag = mass * (1.0 - jnp.exp(-coef[1] * jnp.sqrt(1.0 + square)))
        out = [evapor]
        out += [evapor * coef[2 + j] * speed[j] + drag * slip[j] for j in range(3)]
        out += [evapor * energy]
        for c in range(5):
            high, low = split(out[c])
            src[c] = high
            src[5 + c] = low

        for i in range(ROWS):
            in_row = xs == cell_of(i) // slab_y
            spread = [jnp.where(in_row, src[c, i : i + 1], 0.0).astype(BF16) for c in range(10)]
            total[...] += lax.dot_general(
                jnp.concatenate(spread, axis=0),
                spot[:, i * capacity : (i + 1) * capacity],
                NT,
                preferred_element_type=F32,
            )
        return unused

    lax.fori_loop(0, devices // ROWS, group, 0)
    half = 5 * slab_x
    out_ref[...] = (total[:half] + total[half:]).reshape(5, slab_x, slab_y)


def with_halo(deposit):
    pieces = []
    for axis, dim in (("gx", 1), ("gy", 2)):
        devices, length = (lax.axis_size(axis), deposit.shape[dim])
        up = [(i, i + 1) for i in range(devices - 1)]
        down = [(j, i) for i, j in up]
        last = lax.slice_in_dim(deposit, length - 1, length, axis=dim)
        leading = lax.slice_in_dim(deposit, 0, 1, axis=dim)
        before = lax.ppermute(last, axis, up)
        after = lax.ppermute(leading, axis, down)
        pieces.append(
            jnp.concatenate([before, lax.slice_in_dim(deposit, 0, length - 1, axis=dim)], axis=dim)
            + jnp.concatenate([lax.slice_in_dim(deposit, 1, length, axis=dim), after], axis=dim)
        )
    return pieces[0] + pieces[1]


def per_device(
    parcel_props, size_class, dest_owner, dest_local, class_table, gas_density, gas_rest
):
    devices = lax.axis_size("gx") * lax.axis_size("gy")
    props_count, parcels = parcel_props.shape
    slab_x, slab_y = gas_density.shape
    capacity = -(-max(2, 4 * parcels // devices) // LANES) * LANES
    vmem = pl.BlockSpec(memory_space=pltpu.VMEM)
    smem = pl.BlockSpec(memory_space=pltpu.SMEM)
    packed = pl.pallas_call(
        functools.partial(bucket_kernel, devices, capacity),
        out_shape=jax.ShapeDtypeStruct((devices, ROWS, capacity), F32),
        in_specs=[vmem] * 5,
        out_specs=vmem,
        scratch_shapes=[
            pltpu.VMEM((capacity, parcels), BF16),
            pltpu.VMEM((2 * ROWS, parcels), F32),
        ],
    )(
        parcel_props,
        size_class.reshape(1, parcels),
        dest_owner.reshape(1, parcels),
        dest_local.reshape(1, parcels),
        class_table,
    )
    got = lax.all_to_all(packed, ("gx", "gy"), split_axis=0, concat_axis=0, tiled=True)
    deposit = pl.pallas_call(
        functools.partial(deposit_kernel, devices, capacity),
        out_shape=jax.ShapeDtypeStruct((5, slab_x, slab_y), F32),
        in_specs=[vmem, smem, vmem, vmem],
        out_specs=vmem,
        scratch_shapes=[
            pltpu.VMEM((slab_y, ROWS * capacity), BF16),
            pltpu.VMEM((5, ROWS, capacity), F32),
            pltpu.VMEM((10, ROWS, capacity), F32),
            pltpu.VMEM((10 * slab_x, slab_y), F32),
        ],
    )(got, class_table, gas_density, gas_rest)
    smooth = 0.4 * deposit + 0.15 * with_halo(deposit)
    return (gas_density + smooth[0], gas_rest + smooth[1:])


def solution(mesh):
    return jax.shard_map(
        per_device,
        mesh=mesh,
        in_specs=(
            P(None, ("gx", "gy")),
            P(("gx", "gy")),
            P(("gx", "gy"), None),
            P(("gx", "gy")),
            P(),
            P("gx", "gy"),
            P(None, "gx", "gy"),
        ),
        out_specs=(P("gx", "gy"), P(None, "gx", "gy")),
        check_vma=False,
    )
```

```python
import functools

import jax
import jax.numpy as jnp
from jax import lax
from jax.experimental import pallas as pl
from jax.experimental.pallas import tpu as pltpu
from jax.sharding import PartitionSpec as P

F32 = jnp.float32
BF16 = jnp.bfloat16
LANES = 128
ROWS = 8
NT = (((1,), (1,)), ((), ()))


def split(x):
    high = x.astype(BF16).astype(F32)
    return high, x - high


def iota(shape, dim):
    return lax.broadcasted_iota(jnp.int32, shape, dim)


def fused_kernel(
    width_x,
    width_y,
    capacity,
    props_ref,
    class_ref,
    owner_ref,
    cell_ref,
    table_ref,
    scalars_ref,
    dens_ref,
    rest_ref,
    new_dens_ref,
    new_rest_ref,
    hot,
    vals,
    packed,
    got,
    spot,
    gas,
    src,
    total,
    row_out,
    row_in,
    col_out,
    col_in,
    send_sem,
    recv_sem,
    halo_send,
    halo_recv,
):
    devices = width_x * width_y
    groups = devices // ROWS
    my_x, my_y = lax.axis_index("gx"), lax.axis_index("gy")
    me = my_x * width_y + my_y
    props_count, parcels = props_ref.shape
    classes = table_ref.shape[0]
    slab_x, slab_y = dens_ref.shape

    def place(device):
        return (device // width_y, device % width_y)

    barrier = pltpu.get_barrier_semaphore()

    def greet(k, unused):
        pl.semaphore_signal(
            barrier,
            inc=1,
            device_id=place((me + k) % devices),
            device_id_type=pl.DeviceIdType.MESH,
        )
        return unused

    lax.fori_loop(1, devices, greet, 0)

    def group_at(step):
        turn = (1 - 2 * (step % 2)) * ((step + 1) // 2)
        return (me // ROWS + groups // 2 + turn + groups) % groups

    def copy_to(device):
        return pltpu.make_async_remote_copy(
            src_ref=packed.at[device],
            dst_ref=got.at[me],
            send_sem=send_sem.at[device],
            recv_sem=recv_sem.at[me],
            device_id=place(device),
            device_id_type=pl.DeviceIdType.MESH,
        )

    def copy_from(device):
        return pltpu.make_async_remote_copy(
            src_ref=packed.at[device],
            dst_ref=got.at[device],
            send_sem=send_sem.at[device],
            recv_sem=recv_sem.at[device],
            device_id=place(device),
            device_id_type=pl.DeviceIdType.MESH,
        )

    row, col = (iota((LANES, 2 * LANES), 0), iota((LANES, 2 * LANES), 1))
    upper = jnp.where((col >= LANES) | (row < col), 1.0, 0.0).astype(BF16)
    ids = iota((devices, LANES), 0)
    ranks = iota((capacity, LANES), 0)
    carry = jnp.zeros((devices, LANES), F32)
    for c in range(parcels // LANES):
        mine = owner_ref[:, c * LANES : (c + 1) * LANES] == ids
        counted = jnp.dot(
            jnp.where(mine, 1.0, 0.0).astype(BF16), upper, preferred_element_type=F32
        )
        rank = jnp.sum(
            jnp.where(mine, counted[:, :LANES] + carry, 0.0), axis=0, keepdims=True
        ).astype(jnp.int32)
        carry = carry + counted[:, LANES:]
        hot[:, c * LANES : (c + 1) * LANES] = jnp.where(ranks == rank, 1.0, 0.0).astype(BF16)

    eye = jnp.where(
        iota((props_count, props_count), 0) == iota((props_count, props_count), 1), 1.0, 0.0
    ).astype(BF16)
    table = jnp.concatenate(split(table_ref[...]), axis=0).astype(BF16)
    turned = lax.dot_general(eye, table, NT, preferred_element_type=F32).astype(BF16)
    picks = jnp.where(class_ref[...] == iota((classes, parcels), 0), 1.0, 0.0)
    picks = jnp.concatenate([picks, picks], axis=0).astype(BF16)
    coef = jnp.dot(turned, picks, preferred_element_type=F32)
    props = props_ref[...]
    which = iota((props_count, parcels), 0)
    weights = jnp.where(which >= 5, coef, jnp.where(which == 4, 1.0, 0.0))
    heat_sum = jnp.sum(weights * props, axis=0, keepdims=True)
    which = iota((ROWS, parcels), 0)
    mixed = jnp.where(which == 0, jnp.exp(0.5 * props[0:1]), props[0:ROWS])
    mixed = jnp.where(which == 5, heat_sum, mixed)
    mixed = jnp.where(which == 6, class_ref[...].astype(F32), mixed)
    mixed = jnp.where(which == 7, cell_ref[...].astype(F32), mixed)
    vals[...] = jnp.concatenate(split(mixed), axis=0)

    pl.semaphore_wait(barrier, devices - 1)

    def send_group(step, unused):
        first = group_at(step) * ROWS
        sends = [
            jnp.where(owner_ref[...] == first + i, vals[...], 0.0).astype(BF16)
            for i in range(ROWS)
        ]
        both = lax.dot_general(
            jnp.concatenate(sends, axis=0), hot[...], NT, preferred_element_type=F32
        )
        for i in range(ROWS):
            at = 2 * ROWS * i
            packed[first + i] = both[at : at + ROWS] + both[at + ROWS : at + 2 * ROWS]

        def launch(i, carried):
            device = first + i

            @pl.when(device != me)
            def _():
                copy_to(device).start()

            return carried

        return lax.fori_loop(0, ROWS, launch, unused)

    lax.fori_loop(0, groups, send_group, 0)
    got[me] = packed[me]

    fields = jnp.concatenate([dens_ref[...], rest_ref[...].reshape(4 * slab_x, slab_y)], axis=0)
    tab = jnp.concatenate(split(fields), axis=1).astype(BF16)
    total[...] = jnp.zeros_like(total)
    ys = iota((slab_y, capacity), 0)
    xs = iota((slab_x, capacity), 0)

    def take_group(step, unused):
        first = group_at(step) * ROWS

        def arrive(i, carried):
            @pl.when(first + i != me)
            def _():
                copy_from(first + i).wait_recv()

            return carried

        lax.fori_loop(0, ROWS, arrive, 0)

        def cell_of(i):
            return got[first + i][7:8].astype(jnp.int32)

        def part(c):
            return jnp.concatenate([got[first + i][c : c + 1] for i in range(ROWS)], axis=0)

        for i in range(ROWS):
            cell = cell_of(i)
            lane_hot = jnp.where(ys == cell % slab_y, 1.0, 0.0).astype(BF16)
            spot[:, i * capacity : (i + 1) * capacity] = lane_hot
            found = jnp.dot(
                tab, jnp.concatenate([lane_hot, lane_hot], axis=0), preferred_element_type=F32
            )
            in_row = xs == cell // slab_y
            for c in range(5):
                gas[c, i : i + 1] = jnp.sum(
                    jnp.where(in_row, found[c * slab_x : (c + 1) * slab_x], 0.0),
                    axis=0,
                    keepdims=True,
                )

        kind = part(6).astype(jnp.int32)
        coefs = [jnp.full(kind.shape, scalars_ref[0, j], F32) for j in range(5)]
        for k in range(1, classes):
            same = kind == k
            coefs = [jnp.where(same, scalars_ref[k, j], coefs[j]) for j in range(5)]
        mass = part(0)
        speed = [part(j) for j in (1, 2, 3)]
        heat, energy = part(4), part(5)
        inverse = 1.0 / gas[0]
        slip = [speed[j] - gas[j + 1] * inverse for j in range(3)]
        excess = heat - gas[4] * inverse
        soft = jnp.maximum(excess, 0.0) + jnp.log1p(jnp.exp(-jnp.abs(excess)))
        evapor = mass * (1.0 - jnp.exp(-(coefs[0] * soft)))
        square = slip[0] * slip[0] + slip[1] * slip[1] + slip[2] * slip[2]
        drag = mass * (1.0 - jnp.exp(-coefs[1] * jnp.sqrt(1.0 + square)))
        out = [evapor]
        out += [evapor * coefs[2 + j] * speed[j] + drag * slip[j] for j in range(3)]
        out += [evapor * energy]
        for c in range(5):
            high, low = split(out[c])
            src[c] = high
            src[5 + c] = low

        for i in range(ROWS):
            in_row = xs == cell_of(i) // slab_y
            spread = [jnp.where(in_row, src[c, i : i + 1], 0.0).astype(BF16) for c in range(10)]
            total[...] += lax.dot_general(
                jnp.concatenate(spread, axis=0),
                spot[:, i * capacity : (i + 1) * capacity],
                NT,
                preferred_element_type=F32,
            )
        return unused

    lax.fori_loop(0, groups, take_group, 0)

    half = 5 * slab_x
    deposit = [
        total[c * slab_x : (c + 1) * slab_x]
        + total[half + c * slab_x : half + (c + 1) * slab_x]
        for c in range(5)
    ]
    lane = iota((slab_x, slab_y), 1)
    low_edge = jnp.zeros((slab_x, slab_y), F32)
    high_edge = jnp.zeros((slab_x, slab_y), F32)
    row_out[...] = jnp.zeros_like(row_out)
    for c in range(5):
        row_out[0, c : c + 1] = deposit[c][0:1]
        row_out[1, c : c + 1] = deposit[c][slab_x - 1 : slab_x]
        low_edge = jnp.where(
            lane == c, pltpu.roll(deposit[c], c, 1) if c else deposit[c], low_edge
        )
        high_edge = jnp.where(lane == c, pltpu.roll(deposit[c], c + 1, 1), high_edge)
    col_out[0] = low_edge
    col_out[1] = high_edge

    def edge(out_ref, in_ref, side, base, target):
        return pltpu.make_async_remote_copy(
            src_ref=out_ref.at[side],
            dst_ref=in_ref.at[side],
            send_sem=halo_send.at[base + side],
            recv_sem=halo_recv.at[base + side],
            device_id=target,
            device_id_type=pl.DeviceIdType.MESH,
        )

    edges = [
        (row_out, row_in, 0, 0, (my_x - 1, my_y), my_x > 0, my_x < width_x - 1),
        (row_out, row_in, 1, 0, (my_x + 1, my_y), my_x < width_x - 1, my_x > 0),
        (col_out, col_in, 0, 2, (my_x, my_y - 1), my_y > 0, my_y < width_y - 1),
        (col_out, col_in, 1, 2, (my_x, my_y + 1), my_y < width_y - 1, my_y > 0),
    ]
    for out_ref, in_ref, side, base, target, sends, takes in edges:

        @pl.when(sends)
        def _(out_ref=out_ref, in_ref=in_ref, side=side, base=base, target=target):
            edge(out_ref, in_ref, side, base, target).start()

        @pl.when(jnp.logical_not(takes))
        def _(in_ref=in_ref, side=side):
            in_ref[side] = jnp.zeros(in_ref.shape[1:], F32)

    def wait_sent(k, unused):
        copy_to((me + k) % devices).wait_send()
        return unused

    lax.fori_loop(1, devices, wait_sent, 0)
    for out_ref, in_ref, side, base, target, sends, takes in edges:

        @pl.when(takes)
        def _(out_ref=out_ref, in_ref=in_ref, side=side, base=base, target=target):
            edge(out_ref, in_ref, side, base, target).wait_recv()

    for c in range(5):
        here = deposit[c]
        above = jnp.concatenate([row_in[1, c : c + 1], here[: slab_x - 1]], axis=0)
        below = jnp.concatenate([here[1:], row_in[0, c : c + 1]], axis=0)
        left_in = pltpu.roll(col_in[1], slab_y - c, 1) if c else col_in[1]
        left = jnp.where(lane == 0, left_in, pltpu.roll(here, 1, 1))
        right = jnp.where(
            lane == slab_y - 1,
            pltpu.roll(col_in[0], slab_y - 1 - c, 1),
            pltpu.roll(here, slab_y - 1, 1),
        )
        smooth = 0.4 * here + 0.15 * (below + above + right + left)
        if c == 0:
            new_dens_ref[...] = dens_ref[...] + smooth
        else:
            new_rest_ref[c - 1] = rest_ref[c - 1] + smooth

    for out_ref, in_ref, side, base, target, sends, takes in edges:

        @pl.when(sends)
        def _(out_ref=out_ref, in_ref=in_ref, side=side, base=base, target=target):
            edge(out_ref, in_ref, side, base, target).wait_send()


def per_device(
    parcel_props, size_class, dest_owner, dest_local, class_table, gas_density, gas_rest
):
    width_x, width_y = lax.axis_size("gx"), lax.axis_size("gy")
    devices = width_x * width_y
    props_count, parcels = parcel_props.shape
    slab_x, slab_y = gas_density.shape
    capacity = -(-max(2, 4 * parcels // devices) // LANES) * LANES
    vmem = pl.BlockSpec(memory_space=pltpu.VMEM)
    smem = pl.BlockSpec(memory_space=pltpu.SMEM)
    return pl.pallas_call(
        functools.partial(fused_kernel, width_x, width_y, capacity),
        out_shape=(
            jax.ShapeDtypeStruct(gas_density.shape, F32),
            jax.ShapeDtypeStruct(gas_rest.shape, F32),
        ),
        in_specs=[vmem] * 5 + [smem] + [vmem] * 2,
        out_specs=(vmem, vmem),
        scratch_shapes=[
            pltpu.VMEM((capacity, parcels), BF16),
            pltpu.VMEM((2 * ROWS, parcels), F32),
            pltpu.VMEM((devices, ROWS, capacity), F32),
            pltpu.VMEM((devices, ROWS, capacity), F32),
            pltpu.VMEM((slab_y, ROWS * capacity), BF16),
            pltpu.VMEM((5, ROWS, capacity), F32),
            pltpu.VMEM((10, ROWS, capacity), F32),
            pltpu.VMEM((10 * slab_x, slab_y), F32),
            pltpu.VMEM((2, ROWS, slab_y), F32),
            pltpu.VMEM((2, ROWS, slab_y), F32),
            pltpu.VMEM((2, slab_x, slab_y), F32),
            pltpu.VMEM((2, slab_x, slab_y), F32),
            pltpu.SemaphoreType.DMA((devices,)),
            pltpu.SemaphoreType.DMA((devices,)),
            pltpu.SemaphoreType.DMA((4,)),
            pltpu.SemaphoreType.DMA((4,)),
        ],
        compiler_params=pltpu.CompilerParams(collective_id=0, has_side_effects=True),
    )(
        parcel_props,
        size_class.reshape(1, parcels),
        dest_owner.reshape(1, parcels),
        dest_local.reshape(1, parcels),
        class_table,
        class_table,
        gas_density,
        gas_rest,
    )


def solution(mesh):
    return jax.shard_map(
        per_device,
        mesh=mesh,
        in_specs=(
            P(None, ("gx", "gy")),
            P(("gx", "gy")),
            P(("gx", "gy"), None),
            P(("gx", "gy")),
            P(),
            P("gx", "gy"),
            P(None, "gx", "gy"),
        ),
        out_specs=(P("gx", "gy"), P(None, "gx", "gy")),
        check_vma=False,
    )
```

```python
import functools

import jax
import jax.numpy as jnp
from jax import lax
from jax.experimental import pallas as pl
from jax.experimental.pallas import tpu as pltpu
from jax.sharding import PartitionSpec as P

F32 = jnp.float32
BF16 = jnp.bfloat16
LANES = 128
ROWS = 8
BATCH = 16
NT = (((1,), (1,)), ((), ()))


def split(x):
    high = x.astype(BF16).astype(F32)
    return high, x - high


def iota(shape, dim):
    return lax.broadcasted_iota(jnp.int32, shape, dim)


def fused_kernel(
    width_x,
    width_y,
    capacity,
    props_ref,
    class_ref,
    owner_ref,
    cell_ref,
    table_ref,
    scalars_ref,
    dens_ref,
    rest_ref,
    smooth_ref,
    hot,
    vals,
    owners,
    packed,
    got,
    spot,
    gas,
    src,
    total,
    row_out,
    row_in,
    col_out,
    col_in,
    send_sem,
    recv_sem,
    halo_send,
    halo_recv,
):
    devices = width_x * width_y
    groups = devices // ROWS
    batch = BATCH
    my_x, my_y = lax.axis_index("gx"), lax.axis_index("gy")
    me = my_x * width_y + my_y
    props_count, parcels = props_ref.shape
    classes = table_ref.shape[0]
    slab_x, slab_y = dens_ref.shape

    def place(device):
        return (device // width_y, device % width_y)

    barrier = pltpu.get_barrier_semaphore()

    def greet(k, unused):
        pl.semaphore_signal(
            barrier,
            inc=1,
            device_id=place((me + k) % devices),
            device_id_type=pl.DeviceIdType.MESH,
        )
        return unused

    lax.fori_loop(1, devices, greet, 0)

    def group_at(step):
        turn = (1 - 2 * (step % 2)) * ((step + 1) // 2)
        return (me // ROWS + groups // 2 + turn + groups) % groups

    def copy_to(device):
        return pltpu.make_async_remote_copy(
            src_ref=packed.at[device],
            dst_ref=got.at[me],
            send_sem=send_sem.at[device],
            recv_sem=recv_sem.at[me],
            device_id=place(device),
            device_id_type=pl.DeviceIdType.MESH,
        )

    def copy_from(device):
        return pltpu.make_async_remote_copy(
            src_ref=packed.at[device],
            dst_ref=got.at[device],
            send_sem=send_sem.at[device],
            recv_sem=recv_sem.at[device],
            device_id=place(device),
            device_id_type=pl.DeviceIdType.MESH,
        )

    row, col = (iota((LANES, 2 * LANES), 0), iota((LANES, 2 * LANES), 1))
    upper = jnp.where((col >= LANES) | (row < col), 1.0, 0.0).astype(BF16)
    ids = iota((devices, LANES), 0)
    wide = min(capacity, 256)
    ranks = iota((wide, LANES), 0).astype(F32).astype(BF16)
    one, zero = jnp.ones((), BF16), jnp.zeros((), BF16)
    carry = jnp.zeros((devices, LANES), F32)
    for c in range(parcels // LANES):
        mine = owner_ref[:, c * LANES : (c + 1) * LANES] == ids
        counted = jnp.dot(
            jnp.where(mine, 1.0, 0.0).astype(BF16), upper, preferred_element_type=F32
        )
        rank = jnp.sum(
            jnp.where(mine, counted[:, :LANES] + carry, 0.0), axis=0, keepdims=True
        )
        carry = carry + counted[:, LANES:]
        for start in range(0, capacity, wide):
            local = jnp.clip(rank - start, -1.0, 256.0).astype(BF16)
            hot[start : start + wide, c * LANES : (c + 1) * LANES] = jnp.where(
                ranks == local, one, zero
            )

    eye = jnp.where(
        iota((props_count, props_count), 0) == iota((props_count, props_count), 1), 1.0, 0.0
    ).astype(BF16)
    table = jnp.concatenate(split(table_ref[...]), axis=0).astype(BF16)
    turned = lax.dot_general(eye, table, NT, preferred_element_type=F32).astype(BF16)
    picks = jnp.where(class_ref[...] == iota((classes, parcels), 0), 1.0, 0.0)
    picks = jnp.concatenate([picks, picks], axis=0).astype(BF16)
    coef = jnp.dot(turned, picks, preferred_element_type=F32)
    props = props_ref[...]
    which = iota((props_count, parcels), 0)
    weights = jnp.where(which >= 5, coef, jnp.where(which == 4, 1.0, 0.0))
    heat_sum = jnp.sum(weights * props, axis=0, keepdims=True)
    which = iota((ROWS, parcels), 0)
    mixed = jnp.where(which == 0, jnp.exp(0.5 * props[0:1]), props[0:ROWS])
    mixed = jnp.where(which == 5, heat_sum, mixed)
    mixed = jnp.where(which == 6, class_ref[...].astype(F32), mixed)
    mixed = jnp.where(which == 7, cell_ref[...].astype(F32), mixed)
    vals[...] = jnp.concatenate(split(mixed), axis=0).astype(BF16)
    owners[...] = jnp.broadcast_to(
        owner_ref[...].astype(F32), (2 * ROWS, parcels)
    ).astype(BF16)

    pl.semaphore_wait(barrier, devices - 1)

    def send_group(step, unused):
        first = (me // batch + devices // batch // 2 + step) % (devices // batch) * batch
        sends = [
            jnp.where(
                owners[...] == (first + i).astype(F32).astype(BF16), vals[...], zero
            )
            for i in range(batch)
        ]
        both = lax.dot_general(
            jnp.concatenate(sends, axis=0), hot[...], NT, preferred_element_type=F32
        )
        for i in range(batch):
            at = 2 * ROWS * i
            packed[first + i] = both[at : at + ROWS] + both[at + ROWS : at + 2 * ROWS]

        def launch(i, carried):
            device = first + i

            @pl.when(device != me)
            def _():
                copy_to(device).start()

            return carried

        return lax.fori_loop(0, batch, launch, unused)

    lax.fori_loop(0, devices // batch, send_group, 0)
    got[me] = packed[me]

    fields = jnp.concatenate([dens_ref[...], rest_ref[...].reshape(4 * slab_x, slab_y)], axis=0)
    tab = jnp.concatenate(split(fields), axis=1).astype(BF16)
    total[...] = jnp.zeros_like(total)
    ys = iota((slab_y, capacity), 0).astype(F32).astype(BF16)
    xs = iota((slab_x, capacity), 0)

    def take_group(step, unused):
        first = group_at(step) * ROWS

        def arrive(i, carried):
            @pl.when(first + i != me)
            def _():
                copy_from(first + i).wait_recv()

            return carried

        lax.fori_loop(0, ROWS, arrive, 0)

        def cell_of(i):
            return got[first + i][7:8].astype(jnp.int32)

        def part(c):
            return jnp.concatenate([got[first + i][c : c + 1] for i in range(ROWS)], axis=0)

        for i in range(ROWS):
            cell = cell_of(i)
            lane_hot = jnp.where(
                ys == (cell % slab_y).astype(F32).astype(BF16), one, zero
            )
            spot[:, i * capacity : (i + 1) * capacity] = lane_hot
            found = jnp.dot(
                tab, jnp.concatenate([lane_hot, lane_hot], axis=0), preferred_element_type=F32
            )
            in_row = xs == cell // slab_y
            for c in range(5):
                gas[c, i : i + 1] = jnp.sum(
                    jnp.where(in_row, found[c * slab_x : (c + 1) * slab_x], 0.0),
                    axis=0,
                    keepdims=True,
                )

        kind = part(6).astype(jnp.int32)
        coefs = [jnp.full(kind.shape, scalars_ref[0, j], F32) for j in range(5)]
        for k in range(1, classes):
            same = kind == k
            coefs = [jnp.where(same, scalars_ref[k, j], coefs[j]) for j in range(5)]
        mass = part(0)
        speed = [part(j) for j in (1, 2, 3)]
        heat, energy = part(4), part(5)
        inverse = 1.0 / gas[0]
        slip = [speed[j] - gas[j + 1] * inverse for j in range(3)]
        excess = heat - gas[4] * inverse
        soft = jnp.maximum(excess, 0.0) + jnp.log1p(jnp.exp(-jnp.abs(excess)))
        evapor = mass * (1.0 - jnp.exp(-(coefs[0] * soft)))
        square = slip[0] * slip[0] + slip[1] * slip[1] + slip[2] * slip[2]
        drag = mass * (1.0 - jnp.exp(-coefs[1] * jnp.sqrt(1.0 + square)))
        out = [evapor]
        out += [evapor * coefs[2 + j] * speed[j] + drag * slip[j] for j in range(3)]
        out += [evapor * energy]
        for c in range(5):
            high, low = split(out[c])
            src[c] = high
            src[5 + c] = low

        for i in range(ROWS):
            in_row = xs == cell_of(i) // slab_y
            spread = [jnp.where(in_row, src[c, i : i + 1], 0.0).astype(BF16) for c in range(10)]
            total[...] += lax.dot_general(
                jnp.concatenate(spread, axis=0),
                spot[:, i * capacity : (i + 1) * capacity],
                NT,
                preferred_element_type=F32,
            )
        return unused

    lax.fori_loop(0, groups, take_group, 0)

    half = 5 * slab_x
    deposit = [
        total[c * slab_x : (c + 1) * slab_x]
        + total[half + c * slab_x : half + (c + 1) * slab_x]
        for c in range(5)
    ]
    lane = iota((slab_x, slab_y), 1)
    low_edge = jnp.zeros((slab_x, slab_y), F32)
    high_edge = jnp.zeros((slab_x, slab_y), F32)
    row_out[...] = jnp.zeros_like(row_out)
    for c in range(5):
        row_out[0, c : c + 1] = deposit[c][0:1]
        row_out[1, c : c + 1] = deposit[c][slab_x - 1 : slab_x]
        low_edge = jnp.where(
            lane == c, pltpu.roll(deposit[c], c, 1) if c else deposit[c], low_edge
        )
        high_edge = jnp.where(lane == c, pltpu.roll(deposit[c], c + 1, 1), high_edge)
    col_out[0] = low_edge
    col_out[1] = high_edge

    def edge(out_ref, in_ref, side, base, target):
        return pltpu.make_async_remote_copy(
            src_ref=out_ref.at[side],
            dst_ref=in_ref.at[side],
            send_sem=halo_send.at[base + side],
            recv_sem=halo_recv.at[base + side],
            device_id=target,
            device_id_type=pl.DeviceIdType.MESH,
        )

    edges = [
        (row_out, row_in, 0, 0, (my_x - 1, my_y), my_x > 0, my_x < width_x - 1),
        (row_out, row_in, 1, 0, (my_x + 1, my_y), my_x < width_x - 1, my_x > 0),
        (col_out, col_in, 0, 2, (my_x, my_y - 1), my_y > 0, my_y < width_y - 1),
        (col_out, col_in, 1, 2, (my_x, my_y + 1), my_y < width_y - 1, my_y > 0),
    ]
    for out_ref, in_ref, side, base, target, sends, takes in edges:

        @pl.when(sends)
        def _(out_ref=out_ref, in_ref=in_ref, side=side, base=base, target=target):
            edge(out_ref, in_ref, side, base, target).start()

        @pl.when(jnp.logical_not(takes))
        def _(in_ref=in_ref, side=side):
            in_ref[side] = jnp.zeros(in_ref.shape[1:], F32)

    def wait_sent(k, unused):
        copy_to((me + k) % devices).wait_send()
        return unused

    lax.fori_loop(1, devices, wait_sent, 0)
    for out_ref, in_ref, side, base, target, sends, takes in edges:

        @pl.when(takes)
        def _(out_ref=out_ref, in_ref=in_ref, side=side, base=base, target=target):
            edge(out_ref, in_ref, side, base, target).wait_recv()

    for c in range(5):
        here = deposit[c]
        above = jnp.concatenate([row_in[1, c : c + 1], here[: slab_x - 1]], axis=0)
        below = jnp.concatenate([here[1:], row_in[0, c : c + 1]], axis=0)
        left_in = pltpu.roll(col_in[1], slab_y - c, 1) if c else col_in[1]
        left = jnp.where(lane == 0, left_in, pltpu.roll(here, 1, 1))
        right = jnp.where(
            lane == slab_y - 1,
            pltpu.roll(col_in[0], slab_y - 1 - c, 1),
            pltpu.roll(here, slab_y - 1, 1),
        )
        smooth = 0.4 * here + 0.15 * (below + above + right + left)
        smooth_ref[c] = smooth

    for out_ref, in_ref, side, base, target, sends, takes in edges:

        @pl.when(sends)
        def _(out_ref=out_ref, in_ref=in_ref, side=side, base=base, target=target):
            edge(out_ref, in_ref, side, base, target).wait_send()


def per_device(
    parcel_props, size_class, dest_owner, dest_local, class_table, gas_density, gas_rest
):
    width_x, width_y = lax.axis_size("gx"), lax.axis_size("gy")
    devices = width_x * width_y
    props_count, parcels = parcel_props.shape
    slab_x, slab_y = gas_density.shape
    capacity = -(-max(2, 4 * parcels // devices) // LANES) * LANES
    vmem = pl.BlockSpec(memory_space=pltpu.VMEM)
    smem = pl.BlockSpec(memory_space=pltpu.SMEM)
    smooth = pl.pallas_call(
        functools.partial(fused_kernel, width_x, width_y, capacity),
        out_shape=jax.ShapeDtypeStruct((5, slab_x, slab_y), F32),
        in_specs=[vmem] * 5 + [smem] + [vmem] * 2,
        out_specs=vmem,
        scratch_shapes=[
            pltpu.VMEM((capacity, parcels), BF16),
            pltpu.VMEM((2 * ROWS, parcels), BF16),
            pltpu.VMEM((2 * ROWS, parcels), BF16),
            pltpu.VMEM((devices, ROWS, capacity), F32),
            pltpu.VMEM((devices, ROWS, capacity), F32),
            pltpu.VMEM((slab_y, ROWS * capacity), BF16),
            pltpu.VMEM((5, ROWS, capacity), F32),
            pltpu.VMEM((10, ROWS, capacity), F32),
            pltpu.VMEM((10 * slab_x, slab_y), F32),
            pltpu.VMEM((2, ROWS, slab_y), F32),
            pltpu.VMEM((2, ROWS, slab_y), F32),
            pltpu.VMEM((2, slab_x, slab_y), F32),
            pltpu.VMEM((2, slab_x, slab_y), F32),
            pltpu.SemaphoreType.DMA((devices,)),
            pltpu.SemaphoreType.DMA((devices,)),
            pltpu.SemaphoreType.DMA((4,)),
            pltpu.SemaphoreType.DMA((4,)),
        ],
        compiler_params=pltpu.CompilerParams(collective_id=0, has_side_effects=True),
    )(
        parcel_props,
        size_class.reshape(1, parcels),
        dest_owner.reshape(1, parcels),
        dest_local.reshape(1, parcels),
        class_table,
        class_table,
        gas_density,
        gas_rest,
    )
    return (gas_density + smooth[0], gas_rest + smooth[1:])


def solution(mesh):
    return jax.shard_map(
        per_device,
        mesh=mesh,
        in_specs=(
            P(None, ("gx", "gy")),
            P(("gx", "gy")),
            P(("gx", "gy"), None),
            P(("gx", "gy")),
            P(),
            P("gx", "gy"),
            P(None, "gx", "gy"),
        ),
        out_specs=(P("gx", "gy"), P(None, "gx", "gy")),
        check_vma=False,
    )
```

```python
import functools

import jax
import jax.numpy as jnp
from jax import lax
from jax.experimental import pallas as pl
from jax.experimental.pallas import tpu as pltpu
from jax.sharding import PartitionSpec as P

F32 = jnp.float32
BF16 = jnp.bfloat16
LANES = 128
ROWS = 8
BATCH = 16
NT = (((1,), (1,)), ((), ()))


def split(x):
    high = x.astype(BF16).astype(F32)
    return high, x - high


def iota(shape, dim):
    return lax.broadcasted_iota(jnp.int32, shape, dim)


def fused_kernel(
    width_x,
    width_y,
    capacity,
    props_ref,
    class_ref,
    owner_ref,
    cell_ref,
    table_ref,
    scalars_ref,
    dens_ref,
    rest_ref,
    smooth_ref,
    hot,
    vals,
    owners,
    packed,
    got,
    spot,
    gas,
    src,
    total,
    row_out,
    row_in,
    col_out,
    col_in,
    send_sem,
    recv_sem,
    halo_send,
    halo_recv,
):
    devices = width_x * width_y
    groups = devices // ROWS
    batch = BATCH
    my_x, my_y = lax.axis_index("gx"), lax.axis_index("gy")
    me = my_x * width_y + my_y
    props_count, parcels = props_ref.shape
    classes = table_ref.shape[0]
    slab_x, slab_y = dens_ref.shape

    def place(device):
        return (device // width_y, device % width_y)

    barrier = pltpu.get_barrier_semaphore()

    def greet(k, unused):
        pl.semaphore_signal(
            barrier,
            inc=1,
            device_id=place((me + k) % devices),
            device_id_type=pl.DeviceIdType.MESH,
        )
        return unused

    lax.fori_loop(1, devices, greet, 0)

    pairs = devices // batch
    plane = me // ROWS
    inner = (plane + 1) // 2 % 2

    def group_at(step):
        pair = (plane // 2 + step // 2) % pairs
        own = (step // 2 == 0).astype(jnp.int32)
        parity = own * (plane % 2) + (1 - own) * (1 - pair % 2)
        return 2 * pair + (parity + step) % 2

    def copy_to(device):
        return pltpu.make_async_remote_copy(
            src_ref=packed.at[device],
            dst_ref=got.at[me],
            send_sem=send_sem.at[device],
            recv_sem=recv_sem.at[me],
            device_id=place(device),
            device_id_type=pl.DeviceIdType.MESH,
        )

    def copy_from(device):
        return pltpu.make_async_remote_copy(
            src_ref=packed.at[device],
            dst_ref=got.at[device],
            send_sem=send_sem.at[device],
            recv_sem=recv_sem.at[device],
            device_id=place(device),
            device_id_type=pl.DeviceIdType.MESH,
        )

    row, col = (iota((LANES, 2 * LANES), 0), iota((LANES, 2 * LANES), 1))
    upper = jnp.where((col >= LANES) | (row < col), 1.0, 0.0).astype(BF16)
    ids = iota((devices, LANES), 0)
    wide = min(capacity, 256)
    ranks = iota((wide, LANES), 0).astype(F32).astype(BF16)
    one, zero = jnp.ones((), BF16), jnp.zeros((), BF16)
    carry = jnp.zeros((devices, LANES), F32)
    for c in range(parcels // LANES):
        mine = owner_ref[:, c * LANES : (c + 1) * LANES] == ids
        counted = jnp.dot(
            jnp.where(mine, 1.0, 0.0).astype(BF16), upper, preferred_element_type=F32
        )
        rank = jnp.sum(
            jnp.where(mine, counted[:, :LANES] + carry, 0.0), axis=0, keepdims=True
        )
        carry = carry + counted[:, LANES:]
        for start in range(0, capacity, wide):
            local = jnp.clip(rank - start, -1.0, 256.0).astype(BF16)
            hot[start : start + wide, c * LANES : (c + 1) * LANES] = jnp.where(
                ranks == local, one, zero
            )

    eye = jnp.where(
        iota((props_count, props_count), 0) == iota((props_count, props_count), 1), 1.0, 0.0
    ).astype(BF16)
    table = jnp.concatenate(split(table_ref[...]), axis=0).astype(BF16)
    turned = lax.dot_general(eye, table, NT, preferred_element_type=F32).astype(BF16)
    picks = jnp.where(class_ref[...] == iota((classes, parcels), 0), 1.0, 0.0)
    picks = jnp.concatenate([picks, picks], axis=0).astype(BF16)
    coef = jnp.dot(turned, picks, preferred_element_type=F32)
    props = props_ref[...]
    which = iota((props_count, parcels), 0)
    weights = jnp.where(which >= 5, coef, jnp.where(which == 4, 1.0, 0.0))
    heat_sum = jnp.sum(weights * props, axis=0, keepdims=True)
    which = iota((ROWS, parcels), 0)
    mixed = jnp.where(which == 0, jnp.exp(0.5 * props[0:1]), props[0:ROWS])
    mixed = jnp.where(which == 5, heat_sum, mixed)
    mixed = jnp.where(which == 6, class_ref[...].astype(F32), mixed)
    mixed = jnp.where(which == 7, cell_ref[...].astype(F32), mixed)
    vals[...] = jnp.concatenate(split(mixed), axis=0).astype(BF16)
    owners[...] = jnp.broadcast_to(
        owner_ref[...].astype(F32), (2 * ROWS, parcels)
    ).astype(BF16)

    pl.semaphore_wait(barrier, devices - 1)

    def send_group(step, unused):
        first = (plane // 2 + pairs // 2 * inner + step) % pairs * batch
        sends = [
            jnp.where(
                owners[...] == (first + i).astype(F32).astype(BF16), vals[...], zero
            )
            for i in range(batch)
        ]
        both = lax.dot_general(
            jnp.concatenate(sends, axis=0), hot[...], NT, preferred_element_type=F32
        )
        for i in range(batch):
            at = 2 * ROWS * i
            packed[first + i] = both[at : at + ROWS] + both[at + ROWS : at + 2 * ROWS]

        def launch(i, carried):
            device = first + (me + i) % batch

            @pl.when(device != me)
            def _():
                copy_to(device).start()

            return carried

        return lax.fori_loop(0, batch, launch, unused)

    lax.fori_loop(0, devices // batch, send_group, 0)
    got[me] = packed[me]

    fields = jnp.concatenate([dens_ref[...], rest_ref[...].reshape(4 * slab_x, slab_y)], axis=0)
    tab = jnp.concatenate(split(fields), axis=1).astype(BF16)
    total[...] = jnp.zeros_like(total)
    ys = iota((slab_y, capacity), 0).astype(F32).astype(BF16)
    xs = iota((slab_x, capacity), 0)

    def take_group(step, unused):
        first = group_at(step) * ROWS

        def arrive(i, carried):
            @pl.when(first + i != me)
            def _():
                copy_from(first + i).wait_recv()

            return carried

        lax.fori_loop(0, ROWS, arrive, 0)

        def cell_of(i):
            return got[first + i][7:8].astype(jnp.int32)

        def part(c):
            return jnp.concatenate([got[first + i][c : c + 1] for i in range(ROWS)], axis=0)

        for i in range(ROWS):
            cell = cell_of(i)
            lane_hot = jnp.where(
                ys == (cell % slab_y).astype(F32).astype(BF16), one, zero
            )
            spot[:, i * capacity : (i + 1) * capacity] = lane_hot
            found = jnp.dot(
                tab, jnp.concatenate([lane_hot, lane_hot], axis=0), preferred_element_type=F32
            )
            in_row = xs == cell // slab_y
            for c in range(5):
                gas[c, i : i + 1] = jnp.sum(
                    jnp.where(in_row, found[c * slab_x : (c + 1) * slab_x], 0.0),
                    axis=0,
                    keepdims=True,
                )

        kind = part(6).astype(jnp.int32)
        coefs = [jnp.full(kind.shape, scalars_ref[0, j], F32) for j in range(5)]
        for k in range(1, classes):
            same = kind == k
            coefs = [jnp.where(same, scalars_ref[k, j], coefs[j]) for j in range(5)]
        mass = part(0)
        speed = [part(j) for j in (1, 2, 3)]
        heat, energy = part(4), part(5)
        inverse = 1.0 / gas[0]
        slip = [speed[j] - gas[j + 1] * inverse for j in range(3)]
        excess = heat - gas[4] * inverse
        soft = jnp.maximum(excess, 0.0) + jnp.log1p(jnp.exp(-jnp.abs(excess)))
        evapor = mass * (1.0 - jnp.exp(-(coefs[0] * soft)))
        square = slip[0] * slip[0] + slip[1] * slip[1] + slip[2] * slip[2]
        drag = mass * (1.0 - jnp.exp(-coefs[1] * jnp.sqrt(1.0 + square)))
        out = [evapor]
        out += [evapor * coefs[2 + j] * speed[j] + drag * slip[j] for j in range(3)]
        out += [evapor * energy]
        for c in range(5):
            high, low = split(out[c])
            src[c] = high
            src[5 + c] = low

        for i in range(ROWS):
            in_row = xs == cell_of(i) // slab_y
            spread = [jnp.where(in_row, src[c, i : i + 1], 0.0).astype(BF16) for c in range(10)]
            total[...] += lax.dot_general(
                jnp.concatenate(spread, axis=0),
                spot[:, i * capacity : (i + 1) * capacity],
                NT,
                preferred_element_type=F32,
            )
        return unused

    lax.fori_loop(0, groups, take_group, 0)

    half = 5 * slab_x
    deposit = [
        total[c * slab_x : (c + 1) * slab_x]
        + total[half + c * slab_x : half + (c + 1) * slab_x]
        for c in range(5)
    ]
    lane = iota((slab_x, slab_y), 1)
    low_edge = jnp.zeros((slab_x, slab_y), F32)
    high_edge = jnp.zeros((slab_x, slab_y), F32)
    row_out[...] = jnp.zeros_like(row_out)
    for c in range(5):
        row_out[0, c : c + 1] = deposit[c][0:1]
        row_out[1, c : c + 1] = deposit[c][slab_x - 1 : slab_x]
        low_edge = jnp.where(
            lane == c, pltpu.roll(deposit[c], c, 1) if c else deposit[c], low_edge
        )
        high_edge = jnp.where(lane == c, pltpu.roll(deposit[c], c + 1, 1), high_edge)
    col_out[0] = low_edge
    col_out[1] = high_edge

    def edge(out_ref, in_ref, side, base, target):
        return pltpu.make_async_remote_copy(
            src_ref=out_ref.at[side],
            dst_ref=in_ref.at[side],
            send_sem=halo_send.at[base + side],
            recv_sem=halo_recv.at[base + side],
            device_id=target,
            device_id_type=pl.DeviceIdType.MESH,
        )

    edges = [
        (row_out, row_in, 0, 0, (my_x - 1, my_y), my_x > 0, my_x < width_x - 1),
        (row_out, row_in, 1, 0, (my_x + 1, my_y), my_x < width_x - 1, my_x > 0),
        (col_out, col_in, 0, 2, (my_x, my_y - 1), my_y > 0, my_y < width_y - 1),
        (col_out, col_in, 1, 2, (my_x, my_y + 1), my_y < width_y - 1, my_y > 0),
    ]
    for out_ref, in_ref, side, base, target, sends, takes in edges:

        @pl.when(sends)
        def _(out_ref=out_ref, in_ref=in_ref, side=side, base=base, target=target):
            edge(out_ref, in_ref, side, base, target).start()

        @pl.when(jnp.logical_not(takes))
        def _(in_ref=in_ref, side=side):
            in_ref[side] = jnp.zeros(in_ref.shape[1:], F32)

    def wait_sent(k, unused):
        copy_to((me + k) % devices).wait_send()
        return unused

    lax.fori_loop(1, devices, wait_sent, 0)
    for out_ref, in_ref, side, base, target, sends, takes in edges:

        @pl.when(takes)
        def _(out_ref=out_ref, in_ref=in_ref, side=side, base=base, target=target):
            edge(out_ref, in_ref, side, base, target).wait_recv()

    for c in range(5):
        here = deposit[c]
        above = jnp.concatenate([row_in[1, c : c + 1], here[: slab_x - 1]], axis=0)
        below = jnp.concatenate([here[1:], row_in[0, c : c + 1]], axis=0)
        left_in = pltpu.roll(col_in[1], slab_y - c, 1) if c else col_in[1]
        left = jnp.where(lane == 0, left_in, pltpu.roll(here, 1, 1))
        right = jnp.where(
            lane == slab_y - 1,
            pltpu.roll(col_in[0], slab_y - 1 - c, 1),
            pltpu.roll(here, slab_y - 1, 1),
        )
        smooth = 0.4 * here + 0.15 * (below + above + right + left)
        smooth_ref[c] = smooth

    for out_ref, in_ref, side, base, target, sends, takes in edges:

        @pl.when(sends)
        def _(out_ref=out_ref, in_ref=in_ref, side=side, base=base, target=target):
            edge(out_ref, in_ref, side, base, target).wait_send()


def per_device(
    parcel_props, size_class, dest_owner, dest_local, class_table, gas_density, gas_rest
):
    width_x, width_y = lax.axis_size("gx"), lax.axis_size("gy")
    devices = width_x * width_y
    props_count, parcels = parcel_props.shape
    slab_x, slab_y = gas_density.shape
    capacity = -(-max(2, 4 * parcels // devices) // LANES) * LANES
    vmem = pl.BlockSpec(memory_space=pltpu.VMEM)
    smem = pl.BlockSpec(memory_space=pltpu.SMEM)
    smooth = pl.pallas_call(
        functools.partial(fused_kernel, width_x, width_y, capacity),
        out_shape=jax.ShapeDtypeStruct((5, slab_x, slab_y), F32),
        in_specs=[vmem] * 5 + [smem] + [vmem] * 2,
        out_specs=vmem,
        scratch_shapes=[
            pltpu.VMEM((capacity, parcels), BF16),
            pltpu.VMEM((2 * ROWS, parcels), BF16),
            pltpu.VMEM((2 * ROWS, parcels), BF16),
            pltpu.VMEM((devices, ROWS, capacity), F32),
            pltpu.VMEM((devices, ROWS, capacity), F32),
            pltpu.VMEM((slab_y, ROWS * capacity), BF16),
            pltpu.VMEM((5, ROWS, capacity), F32),
            pltpu.VMEM((10, ROWS, capacity), F32),
            pltpu.VMEM((10 * slab_x, slab_y), F32),
            pltpu.VMEM((2, ROWS, slab_y), F32),
            pltpu.VMEM((2, ROWS, slab_y), F32),
            pltpu.VMEM((2, slab_x, slab_y), F32),
            pltpu.VMEM((2, slab_x, slab_y), F32),
            pltpu.SemaphoreType.DMA((devices,)),
            pltpu.SemaphoreType.DMA((devices,)),
            pltpu.SemaphoreType.DMA((4,)),
            pltpu.SemaphoreType.DMA((4,)),
        ],
        compiler_params=pltpu.CompilerParams(collective_id=0, has_side_effects=True, vmem_limit_bytes=32 * 1024 * 1024),
    )(
        parcel_props,
        size_class.reshape(1, parcels),
        dest_owner.reshape(1, parcels),
        dest_local.reshape(1, parcels),
        class_table,
        class_table,
        gas_density,
        gas_rest,
    )
    return (gas_density + smooth[0], gas_rest + smooth[1:])


def solution(mesh):
    return jax.shard_map(
        per_device,
        mesh=mesh,
        in_specs=(
            P(None, ("gx", "gy")),
            P(("gx", "gy")),
            P(("gx", "gy"), None),
            P(("gx", "gy")),
            P(),
            P("gx", "gy"),
            P(None, "gx", "gy"),
        ),
        out_specs=(P("gx", "gy"), P(None, "gx", "gy")),
        check_vma=False,
    )
```
